32 devices in a mesh: row: 8 (over y, x, core), col: 4 (over z).
Axes of the slice: x: 2, y: 2, z: 4, core: 2. Of those that a mesh axis runs over, the one named last changes fastest.
Arguments:
- density: float32 [256, 256, 256], P('row', 'col'), may hold values from -5 to 5
- green_octant: float32 [256, 256, 256], P('row', 'col'), may hold values from 0 to 0.25
Outputs:
- potential: float32 [256, 256, 256], P('row', 'col')
The draws below stay inside these ranges and needn't reach their ends.
All inputs are finite; a program needn't handle non-finite values.
Results may differ from the reference program's by a relative error of at most 0.000092.
Values sent between devices are 32-bit elements; how exact they have to be, the bound alone decides.
No kernel may reach another device: no remote copies, remote signals or barrier semaphores. Data moves between devices by JAX's collectives and lax.ppermute only.
A program may use at most 192 MiB of HBM per device.

```python
import math
import jax
import jax.numpy as jnp
from jax import lax

N = 256


def draw_density(key, part):
    noise = jax.random.normal(key, (N, N, N), jnp.float32)
    return jnp.clip(noise, -5.0, 5.0)


def draw_green_octant(key, part):
    coords = jnp.arange(N, dtype=jnp.float32)
    radius = jnp.sqrt(coords[:, None, None] * coords[:, None, None] + coords[None, :, None] * coords[None, :, None] + coords[None, None, :] * coords[None, None, :])
    factor = jnp.exp(jax.random.uniform(key, (N, N, N), jnp.float32, math.log(0.5), math.log(1.5)))
    return factor * jnp.exp(-radius / (N / 4.0)) / (4.0 * math.pi * jnp.maximum(radius, 0.5))


def setup_inputs(seed: int = 0) -> dict:
    streams_of = jax.random.split(jax.random.key(seed), 3)
    return {
        "density": draw_density(jax.random.fold_in(streams_of[2], 71), 0),
        "green_octant": draw_green_octant(jax.random.fold_in(streams_of[2], 71), 0),
    }


def cosine_table(extent, padded):
    positions = jnp.arange(extent, dtype=jnp.int32)[:, None]
    waves = jnp.arange(padded, dtype=jnp.int32)[None, :]
    phases = (positions * waves) % padded
    angles = phases.astype(jnp.float32) * jnp.float32(2.0 * 3.141592653589793 / padded)
    weights = jnp.where(positions == 0, jnp.float32(1.0), jnp.float32(2.0))
    return weights * jnp.cos(angles)


def reference(density, green_octant):
    padded = 2 * N
    table = cosine_table(N, padded)
    half_table = table[:, : N + 1]
    along_z = jnp.dot(green_octant.reshape(N * N, N), half_table, precision=lax.Precision.HIGHEST, preferred_element_type=jnp.float32).reshape(N, N, N + 1)
    along_y = jnp.einsum("ijk,jl->ilk", along_z, table, precision=lax.Precision.HIGHEST)
    kernel_hat = jnp.einsum("ijk,il->ljk", along_y, table, precision=lax.Precision.HIGHEST)
    density_hat = jnp.fft.rfftn(density, s=(padded, padded, padded))
    product = density_hat * kernel_hat
    whole = jnp.fft.irfftn(product, s=(padded, padded, padded))
    return whole[:N, :N, :N].astype(jnp.float32)
```

```python
import numpy as np
import jax
import jax.numpy as jnp
from jax import lax
from jax.experimental import pallas as pl
from jax.experimental.pallas import tpu as pltpu
from jax.sharding import PartitionSpec as P

AXES = ("row", "col")
LANES = 128
BF16 = jnp.bfloat16
F32 = jnp.float32
NN = (((1,), (0,)), ((), ()))
NT = (((1,), (1,)), ((), ()))
TN = (((0,), (0,)), ((), ()))


def split_table(table):
    high = table.astype(np.float32).astype(jnp.bfloat16)
    low = (table - high.astype(np.float64)).astype(np.float32).astype(jnp.bfloat16)
    return high, low


def wave_tables(extent):
    freqs = np.arange(extent)[:, None] + 0.5
    cells = np.arange(extent)[None, :]
    angles = np.pi / extent * freqs * (cells - (extent - 1) / 2)
    waves = np.concatenate([np.cos(angles), np.sin(angles)], axis=0)
    weights = np.where(cells == 0, 1.0, 2.0)
    even = weights * np.cos(np.pi / extent * freqs * cells)
    return waves, even


def split(value):
    high = value.astype(BF16)
    low = (value - high.astype(F32)).astype(BF16)
    return high, low


def dot3(left, right, dims):
    lh, ll = left
    rh, rl = right

    def dot(a, b):
        return lax.dot_general(a, b, dims, preferred_element_type=F32)

    return dot(lh, rh) + (dot(lh, rl) + dot(ll, rh))


def whole(shape):
    return pl.BlockSpec(shape, lambda *_: (0,) * len(shape))


def z_forward(lines, tables, pairs):
    rows, extent = lines.shape
    n_out = tables[0].shape[0] // extent

    def body(x_ref, th_ref, tl_ref, *out_refs):
        step = pl.program_id(0)
        right = split(x_ref[...])
        for o, out_ref in enumerate(out_refs):
            part = slice(o * extent, (o + 1) * extent)
            acc = dot3((th_ref[part, :], tl_ref[part, :]), right, NT)
            for h in range(2):
                out_ref[pl.ds(2 * step + h, extent, stride=pairs), :] = acc[:, h * LANES : (h + 1) * LANES]

    return pl.pallas_call(
        body,
        grid=(pairs // 2,),
        in_specs=[pl.BlockSpec((2 * LANES, extent), lambda i: (i, 0)), whole(tables[0].shape), whole(tables[1].shape)],
        out_specs=[whole((extent * pairs, LANES))] * n_out,
        out_shape=[jax.ShapeDtypeStruct((extent * pairs, LANES), F32)] * n_out,
        cost_estimate=pl.CostEstimate(flops=6 * rows * extent * extent * n_out, transcendentals=0, bytes_accessed=4 * rows * extent * (1 + n_out)),
        name="z_forward",
    )(lines, *tables)


def z_inverse(received, tables, pairs, extent, partial):
    rows = pairs * LANES

    def body(r_ref, th_ref, tl_ref, *rest):
        out_ref = rest[-1]
        step = pl.program_id(0)
        left = jnp.concatenate(
            [r_ref[pl.ds(2 * step + h, extent, stride=pairs), :] for h in range(2)], axis=1
        )
        acc = dot3(split(left), (th_ref[...], tl_ref[...]), TN)
        if partial is not None:
            acc = acc + rest[0][...]
        out_ref[...] = acc

    lines = pl.BlockSpec((2 * LANES, extent), lambda i: (i, 0))
    extra = [] if partial is None else [partial]
    return pl.pallas_call(
        body,
        grid=(pairs // 2,),
        in_specs=[whole(received.shape), whole(tables[0].shape), whole(tables[1].shape)] + [lines] * len(extra),
        out_specs=lines,
        out_shape=jax.ShapeDtypeStruct((rows, extent), F32),
        cost_estimate=pl.CostEstimate(flops=6 * rows * extent * extent, transcendentals=0, bytes_accessed=8 * rows * extent),
        name="z_inverse",
    )(received, *tables, *extra)


def lane_half(shape):
    return lax.broadcasted_iota(jnp.int32, shape, 1) < LANES // 2


def swap(value):
    return pltpu.roll(value, LANES // 2, 1)


def read_plane(ref, plane_ref):
    n_row, n_col, _, pairs, _ = ref.shape
    half_x = n_row * pairs
    mask = lane_half((half_x, LANES))
    for p in range(n_col // 2):
        a = ref[:, 2 * p, 0].reshape(half_x, LANES)
        b = ref[:, 2 * p + 1, 0].reshape(half_x, LANES)
        lanes = slice(p * LANES, (p + 1) * LANES)
        plane_ref[:half_x, lanes] = jnp.where(mask, a, swap(b))
        plane_ref[half_x:, lanes] = jnp.where(mask, swap(a), b)


def write_plane(ref, plane):
    n_row, n_col, _, pairs, _ = ref.shape
    half_x = n_row * pairs
    mask = lane_half((half_x, LANES))
    for p in range(n_col // 2):
        lanes = slice(p * LANES, (p + 1) * LANES)
        q0 = plane[:half_x, lanes]
        q1 = plane[half_x:, lanes]
        ref[:, 2 * p, 0] = jnp.where(mask, q0, swap(q1)).reshape(n_row, pairs, LANES)
        ref[:, 2 * p + 1, 0] = jnp.where(mask, swap(q0), q1).reshape(n_row, pairs, LANES)


def block_of(shape):
    n_row, n_col, _, pairs, lanes = shape
    return pl.BlockSpec((n_row, n_col, 1, pairs, lanes), lambda k: (0, 0, k, 0, 0))


def kernel_planes(received, x_tables, y_tables, extent):
    planes = received.shape[2]
    scaling = 1.0 / float(extent) ** 3

    def body(r_ref, xh, xl, yh, yl, out_ref, plane_ref):
        read_plane(r_ref, plane_ref)
        first = dot3((xh[...], xl[...]), split(plane_ref[...]), NN)
        out_ref[0] = dot3(split(first), (yh[...], yl[...]), NT) * scaling

    tables = (*x_tables, *y_tables)
    return pl.pallas_call(
        body,
        grid=(planes,),
        in_specs=[block_of(received.shape)] + [whole(t.shape) for t in tables],
        out_specs=pl.BlockSpec((1, extent, extent), lambda k: (k, 0, 0)),
        out_shape=jax.ShapeDtypeStruct((planes, extent, extent), F32),
        scratch_shapes=[pltpu.VMEM((extent, extent), F32)],
        cost_estimate=pl.CostEstimate(flops=12 * planes * extent**3, transcendentals=0, bytes_accessed=8 * planes * extent**2),
        name="kernel_planes",
    )(received, *tables)


def convolve_planes(received, kernel, x_tables, y_tables, extent):
    planes = received.shape[2]
    block = LANES

    def body(r_ref, k_ref, xh, xl, yh, yl, out_ref, plane_ref, wh_ref, wl_ref):
        read_plane(r_ref, plane_ref)
        plane = split(plane_ref[...])
        y_table = (yh[...], yl[...])
        for i in range(2 * extent // block):
            rows = slice(i * block, (i + 1) * block)
            start = i * block % extent
            along_x = dot3((xh[rows, :], xl[rows, :]), plane, NN)
            spectrum = dot3(split(along_x), y_table, NT)
            weight = k_ref[0, start : start + block, :]
            spectrum = spectrum * jnp.concatenate([weight, weight], axis=1)
            high, low = split(dot3(split(spectrum), y_table, NN))
            wh_ref[rows, :] = high
            wl_ref[rows, :] = low
        result = dot3((xh[...], xl[...]), (wh_ref[...], wl_ref[...]), TN)
        write_plane(out_ref, result)

    tables = (*x_tables, *y_tables)
    return pl.pallas_call(
        body,
        grid=(planes,),
        in_specs=[block_of(received.shape), pl.BlockSpec((1, extent, extent), lambda k: (k, 0, 0))]
        + [whole(t.shape) for t in tables],
        out_specs=block_of(received.shape),
        out_shape=jax.ShapeDtypeStruct(received.shape, F32),
        scratch_shapes=[
            pltpu.VMEM((extent, extent), F32),
            pltpu.VMEM((2 * extent, extent), BF16),
            pltpu.VMEM((2 * extent, extent), BF16),
        ],
        cost_estimate=pl.CostEstimate(flops=72 * planes * extent**3, transcendentals=0, bytes_accessed=12 * planes * extent**2),
        name="convolve_planes",
    )(received, kernel, *tables)


def solution(mesh):
    n_row, n_col = mesh.shape["row"], mesh.shape["col"]
    n_dev = n_row * n_col

    def on_device(density, green_octant):
        local_x, local_y, extent = density.shape
        pairs = local_x * local_y // LANES
        planes = extent // n_dev
        waves, even = wave_tables(extent)
        order = np.arange(extent).reshape(n_row, pairs, 2).transpose(2, 0, 1).reshape(-1)
        y_waves = split_table(waves)
        x_waves = split_table(waves[:, order])
        y_even = split_table(even)
        x_even = split_table(even[:, order])

        def exchange(value):
            value = value.reshape(n_dev, planes * pairs, LANES)
            return lax.all_to_all(value, AXES, 0, 0)

        def by_plane(value):
            return value.reshape(n_row, n_col, planes, pairs, LANES)

        (green_z,) = z_forward(green_octant.reshape(-1, extent), y_even, pairs)
        green_k = exchange(green_z)
        cos_z, sin_z = z_forward(density.reshape(-1, extent), y_waves, pairs)
        cos_k = exchange(cos_z)
        sin_k = exchange(sin_z)
        kernel = kernel_planes(by_plane(green_k), x_even, y_even, extent)
        cos_p = convolve_planes(by_plane(cos_k), kernel, x_waves, y_waves, extent)
        cos_b = exchange(cos_p)
        sin_p = convolve_planes(by_plane(sin_k), kernel, x_waves, y_waves, extent)
        sin_b = exchange(sin_p)
        cos_t = tuple(t[:extent] for t in y_waves)
        sin_t = tuple(t[extent:] for t in y_waves)
        partial = z_inverse(cos_b.reshape(-1, LANES), cos_t, pairs, extent, None)
        result = z_inverse(sin_b.reshape(-1, LANES), sin_t, pairs, extent, partial)
        return result.reshape(local_x, local_y, extent)

    return jax.shard_map(
        on_device,
        mesh=mesh,
        in_specs=(P("row", "col", None), P("row", "col", None)),
        out_specs=P("row", "col", None),
        check_vma=False,
    )
```

```python
import numpy as np
import jax
import jax.numpy as jnp
from jax import lax
from jax.experimental import pallas as pl
from jax.experimental.pallas import tpu as pltpu
from jax.sharding import PartitionSpec as P

AXES = ("row", "col")
LANES = 128
BF16 = jnp.bfloat16
F32 = jnp.float32
NN = (((1,), (0,)), ((), ()))
NT = (((1,), (1,)), ((), ()))
TN = (((0,), (0,)), ((), ()))


def split_table(table):
    high = table.astype(np.float32).astype(jnp.bfloat16)
    low = (table - high.astype(np.float64)).astype(np.float32).astype(jnp.bfloat16)
    return high, low


def wave_tables(extent):
    freqs = np.arange(extent)[:, None] + 0.5
    cells = np.arange(extent)[None, :]
    angles = np.pi / extent * freqs * (cells - (extent - 1) / 2)
    waves = np.concatenate([np.cos(angles), np.sin(angles)], axis=0)
    weights = np.where(cells == 0, 1.0, 2.0)
    even = weights * np.cos(np.pi / extent * freqs * cells)
    return waves, even


def split(value):
    high = value.astype(BF16)
    low = (value - high.astype(F32)).astype(BF16)
    return high, low


def stack_left(high, low, axis):
    return jnp.concatenate([high, high, low], axis=axis)


def stack_right(high, low, axis):
    return jnp.concatenate([high, low, high], axis=axis)


def dot(left, right, dims):
    return lax.dot_general(left, right, dims, preferred_element_type=F32)


def whole(shape):
    return pl.BlockSpec(shape, lambda *_: (0,) * len(shape))


def z_forward(sources, n_dev, pairs):
    rows, extent = sources[0][0].shape
    planes = extent // n_dev
    width = planes * len(sources)
    per = min(8, pairs)
    n = len(sources)

    def body(*refs):
        out_ref = refs[-1]
        step = pl.program_id(0)
        for g in range(n):
            x_ref, h_ref, l_ref = refs[3 * g : 3 * g + 3]
            right = stack_right(*split(x_ref[...]), 1)
            acc = dot(stack_left(h_ref[...], l_ref[...], 1), right, NT)
            for h in range(per):
                for d in range(n_dev):
                    start = (d * width + g * planes) * pairs + per * step + h
                    out_ref[pl.ds(start, planes, stride=pairs), :] = acc[
                        d * planes : (d + 1) * planes, h * LANES : (h + 1) * LANES
                    ]

    lines = pl.BlockSpec((per * LANES, extent), lambda i: (i, 0))
    table = whole((extent, extent))
    return pl.pallas_call(
        body,
        grid=(pairs // per,),
        in_specs=[lines, table, table] * n,
        out_specs=whole((n_dev * width * pairs, LANES)),
        out_shape=jax.ShapeDtypeStruct((n_dev * width * pairs, LANES), F32),
        cost_estimate=pl.CostEstimate(flops=6 * rows * extent * extent * n, transcendentals=0, bytes_accessed=8 * rows * extent * n),
        name="z_forward",
    )(*[a for source in sources for a in source])


def z_inverse(received, tables, pairs, extent, partial):
    rows = pairs * LANES
    per = min(8, pairs)

    def body(r_ref, h_ref, l_ref, *rest):
        out_ref = rest[-1]
        step = pl.program_id(0)
        left = jnp.concatenate(
            [r_ref[pl.ds(per * step + h, extent, stride=pairs), :] for h in range(per)], axis=1
        )
        acc = dot(stack_right(*split(left), 0), stack_left(h_ref[...], l_ref[...], 0), TN)
        if partial is not None:
            acc = acc + rest[0][...]
        out_ref[...] = acc

    lines = pl.BlockSpec((per * LANES, extent), lambda i: (i, 0))
    extra = [] if partial is None else [partial]
    table = whole((extent, extent))
    return pl.pallas_call(
        body,
        grid=(pairs // per,),
        in_specs=[pl.BlockSpec(memory_space=pltpu.VMEM), table, table] + [lines] * len(extra),
        out_specs=lines,
        out_shape=jax.ShapeDtypeStruct((rows, extent), F32),
        cost_estimate=pl.CostEstimate(flops=6 * rows * extent * extent, transcendentals=0, bytes_accessed=8 * rows * extent),
        name="z_inverse",
    )(received, *tables, *extra)


def lane_half(shape):
    return lax.broadcasted_iota(jnp.int32, shape, 1) < LANES // 2


def swap(value):
    return pltpu.roll(value, LANES // 2, 1)


def read_plane(ref, index, plane_ref):
    n_row, n_col, _, pairs, _ = ref.shape
    half_x = n_row * pairs
    mask = lane_half((half_x, LANES))
    for p in range(n_col // 2):
        a = ref[:, 2 * p, index].reshape(half_x, LANES)
        b = ref[:, 2 * p + 1, index].reshape(half_x, LANES)
        lanes = slice(p * LANES, (p + 1) * LANES)
        plane_ref[:half_x, lanes] = jnp.where(mask, a, swap(b))
        plane_ref[half_x:, lanes] = jnp.where(mask, swap(a), b)


def write_plane(ref, plane):
    n_row, n_col, _, pairs, _ = ref.shape
    half_x = n_row * pairs
    mask = lane_half((half_x, LANES))
    for p in range(n_col // 2):
        lanes = slice(p * LANES, (p + 1) * LANES)
        q0 = plane[:half_x, lanes]
        q1 = plane[half_x:, lanes]
        ref[:, 2 * p, 0] = jnp.where(mask, q0, swap(q1)).reshape(n_row, pairs, LANES)
        ref[:, 2 * p + 1, 0] = jnp.where(mask, swap(q0), q1).reshape(n_row, pairs, LANES)


def kernel_planes(received, offset, planes, x_tables, y_tables, extent):
    scaling = 1.0 / float(extent) ** 3

    def body(r_ref, xh, xl, yh, yl, out_ref, plane_ref):
        read_plane(r_ref, offset + pl.program_id(0), plane_ref)
        first = dot(stack_left(xh[...], xl[...], 1), stack_right(*split(plane_ref[...]), 0), NN)
        second = dot(stack_left(*split(first), 1), stack_right(yh[...], yl[...], 1), NT)
        out_ref[0] = second * scaling

    tables = (*x_tables, *y_tables)
    return pl.pallas_call(
        body,
        grid=(planes,),
        in_specs=[pl.BlockSpec(memory_space=pltpu.VMEM)] + [whole(t.shape) for t in tables],
        out_specs=pl.BlockSpec((1, extent, extent), lambda k: (k, 0, 0)),
        out_shape=jax.ShapeDtypeStruct((planes, extent, extent), F32),
        scratch_shapes=[pltpu.VMEM((extent, extent), F32)],
        cost_estimate=pl.CostEstimate(flops=12 * planes * extent**3, transcendentals=0, bytes_accessed=8 * planes * extent**2),
        name="kernel_planes",
    )(received, *tables)


def convolve_planes(received, offset, kernel, x_tables, xt_tables, y_tables, extent):
    planes = kernel.shape[0]
    n_row, n_col, _, pairs, _ = received.shape

    def body(r_ref, k_ref, xh, xl, th, tl, yh, yl, out_ref, plane_ref):
        read_plane(r_ref, offset + pl.program_id(0), plane_ref)
        along_x = dot(stack_left(xh[...], xl[...], 1), stack_right(*split(plane_ref[...]), 0), NN)
        spectrum = dot(stack_left(*split(along_x), 1), stack_right(yh[...], yl[...], 1), NT)
        weight = k_ref[0]
        weight = jnp.concatenate([weight, weight], axis=1)
        spectrum = spectrum * jnp.concatenate([weight, weight], axis=0)
        along_y = dot(stack_left(*split(spectrum), 1), stack_right(yh[...], yl[...], 0), NN)
        result = dot(stack_left(th[...], tl[...], 1), stack_right(*split(along_y), 0), NN)
        write_plane(out_ref, result)

    tables = (*x_tables, *xt_tables, *y_tables)
    shape = (n_row, n_col, planes, pairs, LANES)
    return pl.pallas_call(
        body,
        grid=(planes,),
        in_specs=[pl.BlockSpec(memory_space=pltpu.VMEM), pl.BlockSpec((1, extent, extent), lambda k: (k, 0, 0))]
        + [whole(t.shape) for t in tables],
        out_specs=pl.BlockSpec((n_row, n_col, 1, pairs, LANES), lambda k: (0, 0, k, 0, 0)),
        out_shape=jax.ShapeDtypeStruct(shape, F32),
        scratch_shapes=[pltpu.VMEM((extent, extent), F32)],
        cost_estimate=pl.CostEstimate(flops=72 * planes * extent**3, transcendentals=0, bytes_accessed=12 * planes * extent**2),
        name="convolve_planes",
    )(received, kernel, *tables)


def solution(mesh):
    n_row, n_col = mesh.shape["row"], mesh.shape["col"]
    n_dev = n_row * n_col

    def on_device(density, green_octant):
        local_x, local_y, extent = density.shape
        pairs = local_x * local_y // LANES
        planes = extent // n_dev
        waves, even = wave_tables(extent)
        order = np.arange(extent).reshape(n_row, pairs, 2).transpose(2, 0, 1).reshape(-1)
        y_waves = split_table(waves)
        x_waves = split_table(waves[:, order])
        xt_waves = split_table(waves[:, order].T)
        y_even = split_table(even)
        x_even = split_table(even[:, order])
        cos_z = split_table(waves[:extent])
        sin_z = split_table(waves[extent:])

        def exchange(value):
            value = lax.all_to_all(value.reshape(n_dev, -1, LANES), AXES, 0, 0)
            return value.reshape(n_row, n_col, -1, pairs, LANES)

        dens = density.reshape(-1, extent)
        green = green_octant.reshape(-1, extent)
        first = exchange(z_forward([(green, *y_even), (dens, *cos_z)], n_dev, pairs))
        second = exchange(z_forward([(dens, *sin_z)], n_dev, pairs))
        kernel = kernel_planes(first, 0, planes, x_even, y_even, extent)
        cos_p = convolve_planes(first, planes, kernel, x_waves, xt_waves, y_waves, extent)
        cos_b = exchange(cos_p)
        sin_p = convolve_planes(second, 0, kernel, x_waves, xt_waves, y_waves, extent)
        sin_b = exchange(sin_p)
        partial = z_inverse(cos_b.reshape(-1, LANES), cos_z, pairs, extent, None)
        result = z_inverse(sin_b.reshape(-1, LANES), sin_z, pairs, extent, partial)
        return result.reshape(local_x, local_y, extent)

    return jax.shard_map(
        on_device,
        mesh=mesh,
        in_specs=(P("row", "col", None), P("row", "col", None)),
        out_specs=P("row", "col", None),
        check_vma=False,
    )
```

```python
import numpy as np
import jax
import jax.numpy as jnp
from jax import lax
from jax.experimental import pallas as pl
from jax.experimental.pallas import tpu as pltpu
from jax.sharding import PartitionSpec as P


ALL = ("row", "col")
LANES = 128
BF16 = jnp.bfloat16
F32 = jnp.float32
NN = (((1,), (0,)), ((), ()))
NT = (((1,), (1,)), ((), ()))
TN = (((0,), (0,)), ((), ()))


def split_table(table):
    high = table.astype(np.float32).astype(jnp.bfloat16)
    low = (table - high.astype(np.float64)).astype(np.float32).astype(jnp.bfloat16)
    return high, low


def wave_tables(extent):
    freqs = np.arange(extent)[:, None] + 0.5
    cells = np.arange(extent)[None, :]
    angles = np.pi / extent * freqs * (cells - (extent - 1) / 2)
    waves = np.concatenate([np.cos(angles), np.sin(angles)], axis=0)
    weights = np.where(cells == 0, 1.0, 2.0)
    even = weights * np.cos(np.pi / extent * freqs * cells)
    return waves, even


def split(value):
    high = value.astype(BF16)
    low = (value - high.astype(F32)).astype(BF16)
    return high, low


def stack_left(high, low, axis):
    return jnp.concatenate([high, high, low], axis=axis)


def stack_right(high, low, axis):
    return jnp.concatenate([high, low, high], axis=axis)


def dot(left, right, dims):
    return lax.dot_general(left, right, dims, preferred_element_type=F32)


def whole(shape):
    return pl.BlockSpec(shape, lambda *_: (0,) * len(shape))


def z_forward(sources, n_dev, pairs):
    rows, extent = sources[0][0].shape
    planes = extent // n_dev
    width = planes * len(sources)
    per = min(8, pairs)
    n = len(sources)

    def body(*refs):
        out_ref = refs[-1]
        step = pl.program_id(0)
        for g in range(n):
            x_ref, h_ref, l_ref = refs[3 * g : 3 * g + 3]
            right = stack_right(*split(x_ref[...]), 1)
            part = slice(sources[g][3], sources[g][3] + extent)
            acc = dot(stack_left(h_ref[part, :], l_ref[part, :], 1), right, NT)
            for h in range(per):
                for d in range(n_dev):
                    start = (d * width + g * planes) * pairs + per * step + h
                    out_ref[pl.ds(start, planes, stride=pairs), :] = acc[
                        d * planes : (d + 1) * planes, h * LANES : (h + 1) * LANES
                    ]

    lines = pl.BlockSpec((per * LANES, extent), lambda i: (i, 0))
    return pl.pallas_call(
        body,
        grid=(pairs // per,),
        in_specs=[s for source in sources for s in (lines, whole(source[1].shape), whole(source[2].shape))],
        out_specs=whole((n_dev * width * pairs, LANES)),
        out_shape=jax.ShapeDtypeStruct((n_dev * width * pairs, LANES), F32),
        cost_estimate=pl.CostEstimate(flops=6 * rows * extent * extent * n, transcendentals=0, bytes_accessed=8 * rows * extent * n),
        name="z_forward",
    )(*[a for source in sources for a in source[:3]])


SCALAR = pl.BlockSpec(memory_space=pltpu.SMEM)
VECTOR = pl.BlockSpec(memory_space=pltpu.VMEM)


def z_inverse(col, received, tables, table_rows, pairs, extent, partial):
    rows = pairs * LANES
    per = min(8, pairs)
    first, last = table_rows
    n_col = tables[0].shape[0]
    n_row = received[-1].shape[0]
    planes = (last - first) // n_row
    received = [r.reshape(-1, LANES) for r in received]

    def body(col_ref, *refs):
        r_refs = refs[: len(received)]
        h_ref, l_ref, *rest = refs[len(received) :]
        out_ref = rest[-1]
        step = pl.program_id(0)

        def block(h, s, j):
            start = j * pairs + per * step + h
            if s > 0 and len(r_refs) > 1:
                return r_refs[s][pl.ds(start, n_row, stride=planes * pairs), :]
            return r_refs[0][pl.ds(s * planes * pairs + start, n_row, stride=n_col * planes * pairs), :]

        left = jnp.concatenate(
            [
                jnp.concatenate([block(h, s, j) for s in range(n_col) for j in range(planes)], axis=0)
                for h in range(per)
            ],
            axis=1,
        )
        source = [lax.rem(col_ref[0] + n_col - s, n_col) for s in range(n_col)]
        high = jnp.concatenate([h_ref[c, first:last] for c in source], axis=0)
        low = jnp.concatenate([l_ref[c, first:last] for c in source], axis=0)
        acc = dot(stack_right(*split(left), 0), stack_left(high, low, 0), TN)
        if partial is not None:
            acc = acc + rest[0][...]
        out_ref[...] = acc

    lines = pl.BlockSpec((per * LANES, extent), lambda i: (i, 0))
    extra = [] if partial is None else [partial]
    return pl.pallas_call(
        body,
        grid=(pairs // per,),
        in_specs=[SCALAR] + [VECTOR] * len(received) + [whole(t.shape) for t in tables] + [lines] * len(extra),
        out_specs=lines,
        out_shape=jax.ShapeDtypeStruct((rows, extent), F32),
        cost_estimate=pl.CostEstimate(
            flops=6 * rows * extent * n_col * (last - first), transcendentals=0, bytes_accessed=8 * rows * extent
        ),
        name="z_inverse",
    )(col, *received, *tables, *extra)


def lane_half(shape):
    return lax.broadcasted_iota(jnp.int32, shape, 1) < LANES // 2


def swap(value):
    return pltpu.roll(value, LANES // 2, 1)


def read_plane(ref, index, plane_ref):
    n_row, n_col, _, pairs, _ = ref.shape
    half_x = n_row * pairs
    mask = lane_half((half_x, LANES))
    for p in range(n_col // 2):
        a = ref[:, 2 * p, index].reshape(half_x, LANES)
        b = ref[:, 2 * p + 1, index].reshape(half_x, LANES)
        plane_ref[p, pl.ds(0, half_x, stride=2)] = jnp.where(mask, a, swap(b))
        plane_ref[p, pl.ds(1, half_x, stride=2)] = jnp.where(mask, swap(a), b)
    return jnp.concatenate([plane_ref[p] for p in range(n_col // 2)], axis=1)


def write_plane(col, plane, plane_ref, block_ref, store):
    n_col = block_ref.shape[0]
    half_x = plane_ref.shape[1] // 2
    mask = lane_half((half_x, LANES))
    for p in range(n_col // 2):
        plane_ref[p] = plane[:, p * LANES : (p + 1) * LANES]
        q0 = plane_ref[p, pl.ds(0, half_x, stride=2)]
        q1 = plane_ref[p, pl.ds(1, half_x, stride=2)]
        block_ref[2 * p] = jnp.where(mask, q0, swap(q1))
        block_ref[2 * p + 1] = jnp.where(mask, swap(q0), q1)
    for s in range(n_col):
        store(s, block_ref[lax.rem(col + s, n_col)])


def kernel_planes(received, planes, tables, extent):
    scaling = 1.0 / float(extent) ** 3

    def body(r_ref, yh, yl, out_ref, plane_ref):
        plane = read_plane(r_ref, pl.program_id(0), plane_ref)
        first = dot(stack_left(yh[...], yl[...], 1), stack_right(*split(plane), 0), NN)
        second = dot(stack_left(*split(first), 1), stack_right(yh[...], yl[...], 1), NT)
        out_ref[0] = second * scaling

    return pl.pallas_call(
        body,
        grid=(planes,),
        in_specs=[VECTOR] + [whole(t.shape) for t in tables],
        out_specs=pl.BlockSpec((1, extent, extent), lambda k: (k, 0, 0)),
        out_shape=jax.ShapeDtypeStruct((planes, extent, extent), F32),
        scratch_shapes=[pltpu.VMEM((extent // LANES, extent, LANES), F32)],
        cost_estimate=pl.CostEstimate(flops=12 * planes * extent**3, transcendentals=0, bytes_accessed=8 * planes * extent**2),
        name="kernel_planes",
    )(received, *tables)


def convolve_planes(col, received, offset, kernel, kernel_offset, planes, joined, t_tables, y_tables, extent):
    n_row, n_col, _, pairs, _ = received.shape

    def body(col_ref, r_ref, k_ref, th, tl, yh, yl, *rest):
        *outs, plane_ref, block_ref = rest
        plane = read_plane(r_ref, offset + pl.program_id(0), plane_ref)
        along_x = dot(stack_left(yh[...], yl[...], 1), stack_right(*split(plane), 0), NN)
        spectrum = dot(stack_left(*split(along_x), 1), stack_right(yh[...], yl[...], 1), NT)
        weight = k_ref[0]
        weight = jnp.concatenate([weight, weight], axis=1)
        spectrum = spectrum * jnp.concatenate([weight, weight], axis=0)
        along_y = dot(stack_left(*split(spectrum), 1), stack_right(yh[...], yl[...], 0), NN)
        result = dot(stack_left(th[...], tl[...], 1), stack_right(*split(along_y), 0), NN)

        def store(s, value):
            value = value.reshape(n_row, pairs, LANES)
            if joined:
                outs[0][:, s, 0] = value
            else:
                outs[s][:, 0] = value

        write_plane(col_ref[0], result, plane_ref, block_ref, store)

    tables = (*t_tables, *y_tables)
    if joined:
        shapes = [(n_row, n_col, planes, pairs, LANES)]
        specs = [pl.BlockSpec((n_row, n_col, 1, pairs, LANES), lambda k: (0, 0, k, 0, 0))]
    else:
        shapes = [(n_row, planes, pairs, LANES)] * n_col
        specs = [pl.BlockSpec((n_row, 1, pairs, LANES), lambda k: (0, k, 0, 0))] * n_col
    return pl.pallas_call(
        body,
        grid=(planes,),
        in_specs=[SCALAR, VECTOR, pl.BlockSpec((1, extent, extent), lambda k: (kernel_offset + k, 0, 0))]
        + [whole(t.shape) for t in tables],
        out_specs=specs,
        out_shape=[jax.ShapeDtypeStruct(s, F32) for s in shapes],
        scratch_shapes=[
            pltpu.VMEM((extent // LANES, extent, LANES), F32),
            pltpu.VMEM((n_col, n_row * pairs, LANES), F32),
        ],
        cost_estimate=pl.CostEstimate(flops=72 * planes * extent**3, transcendentals=0, bytes_accessed=12 * planes * extent**2),
        name="convolve_planes",
    )(col, received, kernel, *tables)


def join(parts):
    n_row, length, _ = parts[0].shape
    block = n_row // 2

    def body(*refs):
        for s, ref in enumerate(refs[:-1]):
            refs[-1][:, s] = ref[...]

    return pl.pallas_call(
        body,
        grid=(n_row // block,),
        in_specs=[pl.BlockSpec((block, length, LANES), lambda i: (i, 0, 0))] * len(parts),
        out_specs=pl.BlockSpec((block, len(parts), length, LANES), lambda i: (i, 0, 0, 0)),
        out_shape=jax.ShapeDtypeStruct((n_row, len(parts), length, LANES), F32),
        name="join",
    )(*parts)


def solution(mesh):
    n_row, n_col = mesh.shape["row"], mesh.shape["col"]
    n_dev = n_row * n_col

    def on_device(density, green_octant):
        local_x, local_y, extent = density.shape
        pairs = local_x * local_y // LANES
        freqs = extent // n_dev
        waves, even = wave_tables(extent)
        y_waves = split_table(waves)
        t_waves = split_table(waves.T)
        y_even = split_table(even)

        def by_owner(table):
            table = table.reshape(n_row, n_col, freqs, extent).transpose(1, 2, 0, 3)
            return table.reshape(n_col, freqs * n_row, extent)

        cos_z = split_table(by_owner(waves[:extent]))
        sin_z = split_table(by_owner(waves[extent:]))
        col = lax.axis_index("col").astype(jnp.int32).reshape(1)

        def exchange(value):
            value = lax.all_to_all(value.reshape(n_dev, -1, LANES), ALL, 0, 0)
            return value.reshape(n_row, n_col, -1, pairs, LANES)

        def spread(value):
            return lax.all_to_all(value.reshape(n_row, n_col, -1, LANES), "row", 0, 0)

        def send(values):
            received = []
            for s, value in enumerate(values, start=1):
                perm = [(c, (c + s) % n_col) for c in range(n_col)]
                received.append(lax.ppermute(value.reshape(n_row, -1, LANES), "col", perm))
            return received

        dens = density.reshape(-1, extent)
        green = green_octant.reshape(-1, extent)
        first = exchange(z_forward([(green, *y_even, 0), (dens, *y_waves, 0)], n_dev, pairs))
        second = exchange(z_forward([(dens, *y_waves, extent)], n_dev, pairs))
        kernel = kernel_planes(first, freqs, y_even, extent)
        own, *others = convolve_planes(col, first, freqs, kernel, 0, freqs, False, t_waves, y_waves, extent)
        others = send(others)
        begin = freqs // 2
        parts = []
        for start, stop in ((0, begin), (begin, freqs)):
            (out,) = convolve_planes(col, second, start, kernel, start, stop - start, True, t_waves, y_waves, extent)
            out = spread(out)
            sent = send([out[:, s] for s in range(1, n_col)])
            parts.append(([out, *sent], (start * n_row, stop * n_row)))
        cos_b = join([own.reshape(n_row, -1, LANES), *others])
        cos_b = lax.all_to_all(cos_b, "row", 0, 0)
        result = z_inverse(col, parts[0][0], sin_z, parts[0][1], pairs, extent, None)
        result = z_inverse(col, [cos_b], cos_z, (0, freqs * n_row), pairs, extent, result)
        result = z_inverse(col, parts[1][0], sin_z, parts[1][1], pairs, extent, result)
        return result.reshape(local_x, local_y, extent)

    spec = P("row", "col", None)
    return jax.shard_map(on_device, mesh=mesh, in_specs=(spec, spec), out_specs=spec, check_vma=False)
```

```python
import numpy as np
import jax
import jax.numpy as jnp
from jax import lax
from jax.experimental import pallas as pl
from jax.experimental.pallas import tpu as pltpu
from jax.sharding import PartitionSpec as P


ALL = ("row", "col")
LANES = 128
BF16 = jnp.bfloat16
F32 = jnp.float32
NN = (((1,), (0,)), ((), ()))
NT = (((1,), (1,)), ((), ()))
TN = (((0,), (0,)), ((), ()))


def split_table(table):
    high = table.astype(np.float32).astype(jnp.bfloat16)
    low = (table - high.astype(np.float64)).astype(np.float32).astype(jnp.bfloat16)
    return high, low


def wave_tables(extent):
    freqs = np.arange(extent)[:, None] + 0.5
    cells = np.arange(extent)[None, :]
    angles = np.pi / extent * freqs * (cells - (extent - 1) / 2)
    waves = np.concatenate([np.cos(angles), np.sin(angles)], axis=0)
    weights = np.where(cells == 0, 1.0, 2.0)
    even = weights * np.cos(np.pi / extent * freqs * cells)
    return waves, even


def split(value):
    high = value.astype(BF16)
    low = (value - high.astype(F32)).astype(BF16)
    return high, low


def stack_left(high, low, axis):
    return jnp.concatenate([high, high, low], axis=axis)


def stack_right(high, low, axis):
    return jnp.concatenate([high, low, high], axis=axis)


def dot(left, right, dims):
    return lax.dot_general(left, right, dims, preferred_element_type=F32)


def whole(shape):
    return pl.BlockSpec(shape, lambda *_: (0,) * len(shape))


SCALAR = pl.BlockSpec(memory_space=pltpu.SMEM)
VECTOR = pl.BlockSpec(memory_space=pltpu.VMEM)


def z_forward(sources, n_dev, pairs):
    rows, extent = sources[0][0].shape
    all_planes = extent // n_dev
    counts = [source[4] for source in sources]
    width = sum(counts)
    per = min(8, pairs)
    n = len(sources)

    def body(*refs):
        out_ref = refs[-1]
        step = pl.program_id(0)
        for g in range(n):
            x_ref, h_ref, l_ref = refs[3 * g : 3 * g + 3]
            right = stack_right(*split(x_ref[...]), 1)
            part = slice(sources[g][3], sources[g][3] + extent)
            acc = dot(stack_left(h_ref[part, :], l_ref[part, :], 1), right, NT)
            for h in range(per):
                for d in range(n_dev):
                    start = (d * width + sum(counts[:g])) * pairs + per * step + h
                    out_ref[pl.ds(start, counts[g], stride=pairs), :] = acc[
                        d * all_planes : d * all_planes + counts[g], h * LANES : (h + 1) * LANES
                    ]

    lines = pl.BlockSpec((per * LANES, extent), lambda i: (i, 0))
    return pl.pallas_call(
        body,
        grid=(pairs // per,),
        in_specs=[s for source in sources for s in (lines, whole(source[1].shape), whole(source[2].shape))],
        out_specs=whole((n_dev * width * pairs, LANES)),
        out_shape=jax.ShapeDtypeStruct((n_dev * width * pairs, LANES), F32),
        cost_estimate=pl.CostEstimate(flops=6 * rows * extent * extent * n, transcendentals=0, bytes_accessed=8 * rows * extent * n),
        name="z_forward",
    )(*[a for source in sources for a in source[:3]])


def z_forward_slots(col, lines, tables, table_rows, n_row, pairs):
    rows, extent = lines.shape
    per = min(8, pairs)
    first, last = table_rows
    n_col = tables[0].shape[0]
    planes = (last - first) // n_row

    def body(col_ref, x_ref, h_ref, l_ref, *out_refs):
        step = pl.program_id(0)
        target = [lax.rem(col_ref[0] + s, n_col) for s in range(n_col)]
        high = jnp.concatenate([h_ref[c, first:last] for c in target], axis=0)
        low = jnp.concatenate([l_ref[c, first:last] for c in target], axis=0)
        acc = dot(stack_left(high, low, 1), stack_right(*split(x_ref[...]), 1), NT)
        for s, out_ref in enumerate(out_refs):
            for j in range(planes):
                row = (s * planes + j) * n_row
                for h in range(per):
                    start = j * pairs + per * step + h
                    out_ref[pl.ds(start, n_row, stride=planes * pairs), :] = acc[
                        row : row + n_row, h * LANES : (h + 1) * LANES
                    ]

    shape = (n_row * planes * pairs, LANES)
    return pl.pallas_call(
        body,
        grid=(pairs // per,),
        in_specs=[SCALAR, pl.BlockSpec((per * LANES, extent), lambda i: (i, 0))] + [whole(t.shape) for t in tables],
        out_specs=[whole(shape)] * n_col,
        out_shape=[jax.ShapeDtypeStruct(shape, F32)] * n_col,
        cost_estimate=pl.CostEstimate(
            flops=6 * rows * extent * n_col * (last - first), transcendentals=0, bytes_accessed=8 * rows * extent
        ),
        name="z_forward_slots",
    )(col, lines, *tables)


def z_inverse(col, groups, n_row, pairs, extent, partial):
    rows = pairs * LANES
    per = min(8, pairs)
    n_col = groups[0][1][0].shape[0]
    counts = [len(received) for received, _, _ in groups]
    depth = n_col * sum(last - first for _, _, (first, last) in groups)

    def body(col_ref, *refs):
        refs = list(refs)
        step = pl.program_id(0)
        source = [lax.rem(col_ref[0] + n_col - s, n_col) for s in range(n_col)]
        columns = [[] for _ in range(per)]
        highs, lows = [], []
        for g, (_, _, (first, last)) in enumerate(groups):
            r_refs = [refs.pop(0) for _ in range(counts[g])]
            h_ref, l_ref = refs.pop(0), refs.pop(0)
            planes = (last - first) // n_row
            for s in range(n_col):
                ref, slots, place = (r_refs[s], 1, 0) if s > 0 and len(r_refs) > 1 else (r_refs[0], n_col, s)
                for j in range(planes):
                    for h in range(per):
                        start = (place * planes + j) * pairs + per * step + h
                        columns[h].append(ref[pl.ds(start, n_row, stride=slots * planes * pairs), :])
                highs.append(h_ref[source[s], first:last])
                lows.append(l_ref[source[s], first:last])
        left = jnp.concatenate([jnp.concatenate(blocks, axis=0) for blocks in columns], axis=1)
        high = jnp.concatenate(highs, axis=0)
        low = jnp.concatenate(lows, axis=0)
        acc = dot(stack_right(*split(left), 0), stack_left(high, low, 0), TN)
        if partial is not None:
            acc = acc + refs[0][...]
        refs[-1][...] = acc

    lines = pl.BlockSpec((per * LANES, extent), lambda i: (i, 0))
    specs, operands = [SCALAR], [col]
    for received, tables, _ in groups:
        specs += [VECTOR] * len(received) + [whole(t.shape) for t in tables]
        operands += [r.reshape(-1, LANES) for r in received] + list(tables)
    if partial is not None:
        specs.append(lines)
        operands.append(partial)
    return pl.pallas_call(
        body,
        grid=(pairs // per,),
        in_specs=specs,
        out_specs=lines,
        out_shape=jax.ShapeDtypeStruct((rows, extent), F32),
        cost_estimate=pl.CostEstimate(
            flops=6 * rows * extent * depth, transcendentals=0, bytes_accessed=8 * rows * extent
        ),
        name="z_inverse",
    )(*operands)


def lane_half(shape):
    return lax.broadcasted_iota(jnp.int32, shape, 1) < LANES // 2


def swap(value):
    return pltpu.roll(value, LANES // 2, 1)


def read_plane(ref, index, plane_ref, slot=lambda c: c):
    n_row, n_col, _, pairs, _ = ref.shape
    half_x = n_row * pairs
    mask = lane_half((half_x, LANES))
    for p in range(n_col // 2):
        a = ref[:, slot(2 * p), index].reshape(half_x, LANES)
        b = ref[:, slot(2 * p + 1), index].reshape(half_x, LANES)
        plane_ref[p, pl.ds(0, half_x, stride=2)] = jnp.where(mask, a, swap(b))
        plane_ref[p, pl.ds(1, half_x, stride=2)] = jnp.where(mask, swap(a), b)
    return jnp.concatenate([plane_ref[p] for p in range(n_col // 2)], axis=1)


def write_plane(col, plane, plane_ref, block_ref, store):
    n_col = block_ref.shape[0]
    half_x = plane_ref.shape[1] // 2
    mask = lane_half((half_x, LANES))
    for p in range(n_col // 2):
        plane_ref[p] = plane[:, p * LANES : (p + 1) * LANES]
        q0 = plane_ref[p, pl.ds(0, half_x, stride=2)]
        q1 = plane_ref[p, pl.ds(1, half_x, stride=2)]
        block_ref[2 * p] = jnp.where(mask, q0, swap(q1))
        block_ref[2 * p + 1] = jnp.where(mask, swap(q0), q1)
    for s in range(n_col):
        store(s, block_ref[lax.rem(col + s, n_col)])


def kernel_planes(received, planes, tables, extent):
    scaling = 1.0 / float(extent) ** 3
    per = min(4, planes)

    def body(r_ref, yh, yl, out_ref, plane_ref):
        for i in range(per):
            plane = read_plane(r_ref, per * pl.program_id(0) + i, plane_ref.at[i])
            first = dot(stack_left(yh[...], yl[...], 1), stack_right(*split(plane), 0), NN)
            second = dot(stack_left(*split(first), 1), stack_right(yh[...], yl[...], 1), NT)
            out_ref[i] = second * scaling

    return pl.pallas_call(
        body,
        grid=(planes // per,),
        in_specs=[VECTOR] + [whole(t.shape) for t in tables],
        out_specs=pl.BlockSpec((per, extent, extent), lambda k: (k, 0, 0)),
        out_shape=jax.ShapeDtypeStruct((planes, extent, extent), F32),
        scratch_shapes=[pltpu.VMEM((per, extent // LANES, extent, LANES), F32)],
        cost_estimate=pl.CostEstimate(flops=12 * planes * extent**3, transcendentals=0, bytes_accessed=8 * planes * extent**2),
        name="kernel_planes",
    )(received, *tables)


def convolve_planes(col, received, relative, offset, kernel, kernel_offset, planes, joined, t_tables, y_tables, extent):
    n_row, n_col, _, pairs, _ = received.shape

    per = 2 if planes % 2 == 0 else 1

    def body(col_ref, r_ref, k_ref, th, tl, yh, yl, *rest):
        *outs, plane_ref, block_ref = rest
        slot = (lambda c: lax.rem(col_ref[0] + (n_col - c), n_col)) if relative else (lambda c: c)
        results = []
        for i in range(per):
            plane = read_plane(r_ref, offset + per * pl.program_id(0) + i, plane_ref.at[i], slot)
            along_x = dot(stack_left(yh[...], yl[...], 1), stack_right(*split(plane), 0), NN)
            weight = jnp.concatenate([k_ref[i], k_ref[i]], axis=1)
            along_y = []
            for part in (along_x[:extent], along_x[extent:]):
                spectrum = dot(stack_left(*split(part), 1), stack_right(yh[...], yl[...], 1), NT) * weight
                along_y.append(dot(stack_left(*split(spectrum), 1), stack_right(yh[...], yl[...], 0), NN))
            along_y = jnp.concatenate(along_y, axis=0)
            results.append(dot(stack_left(th[...], tl[...], 1), stack_right(*split(along_y), 0), NN))

        for i in range(per):

            def store(s, value):
                value = value.reshape(n_row, pairs, LANES)
                if joined:
                    outs[0][:, s, i] = value
                else:
                    outs[s][:, i] = value

            write_plane(col_ref[0], results[i], plane_ref.at[i], block_ref, store)

    tables = (*t_tables, *y_tables)
    if joined:
        shapes = [(n_row, n_col, planes, pairs, LANES)]
        specs = [pl.BlockSpec((n_row, n_col, per, pairs, LANES), lambda k: (0, 0, k, 0, 0))]
    else:
        shapes = [(n_row, planes, pairs, LANES)] * n_col
        specs = [pl.BlockSpec((n_row, per, pairs, LANES), lambda k: (0, k, 0, 0))] * n_col
    return pl.pallas_call(
        body,
        grid=(planes // per,),
        in_specs=[SCALAR, VECTOR, pl.BlockSpec((per, extent, extent), lambda k: (kernel_offset // per + k, 0, 0))]
        + [whole(t.shape) for t in tables],
        out_specs=specs,
        out_shape=[jax.ShapeDtypeStruct(s, F32) for s in shapes],
        scratch_shapes=[
            pltpu.VMEM((per, extent // LANES, extent, LANES), F32),
            pltpu.VMEM((n_col, n_row * pairs, LANES), F32),
        ],
        cost_estimate=pl.CostEstimate(flops=72 * planes * extent**3, transcendentals=0, bytes_accessed=12 * planes * extent**2),
        name="convolve_planes",
    )(col, received, kernel, *tables)


def join(groups):
    n_row = groups[0][0].shape[0]
    lengths = [group[0].shape[1] for group in groups]
    n_slot = len(groups[0])
    block = n_row // 2

    def body(*refs):
        begin = 0
        for g, length in enumerate(lengths):
            for s in range(n_slot):
                refs[-1][:, s, begin : begin + length] = refs[g * n_slot + s][...]
            begin += length

    total = sum(lengths)
    return pl.pallas_call(
        body,
        grid=(n_row // block,),
        in_specs=[pl.BlockSpec((block, n, LANES), lambda i: (i, 0, 0)) for n in lengths for _ in range(n_slot)],
        out_specs=pl.BlockSpec((block, n_slot, total, LANES), lambda i: (i, 0, 0, 0)),
        out_shape=jax.ShapeDtypeStruct((n_row, n_slot, total, LANES), F32),
        name="join",
    )(*[part for group in groups for part in group])


def solution(mesh):
    n_row, n_col = mesh.shape["row"], mesh.shape["col"]
    n_dev = n_row * n_col

    def on_device(density, green_octant):
        local_x, local_y, extent = density.shape
        pairs = local_x * local_y // LANES
        freqs = extent // n_dev
        waves, even = wave_tables(extent)
        y_waves = split_table(waves)
        t_waves = split_table(waves.T)
        y_even = split_table(even)

        def by_owner(table):
            table = table.reshape(n_row, n_col, freqs, extent).transpose(1, 2, 0, 3)
            return table.reshape(n_col, freqs * n_row, extent)

        cos_z = split_table(by_owner(waves[:extent]))
        sin_z = split_table(by_owner(waves[extent:]))
        col = lax.axis_index("col").astype(jnp.int32).reshape(1)

        def exchange(value):
            value = lax.all_to_all(value.reshape(n_dev, -1, LANES), ALL, 0, 0)
            return value.reshape(n_row, n_col, -1, pairs, LANES)

        def spread(value):
            return lax.all_to_all(value.reshape(n_row, n_col, -1, LANES), "row", 0, 0)

        def send(values):
            received = []
            for s, value in enumerate(values, start=1):
                perm = [(c, (c + s) % n_col) for c in range(n_col)]
                received.append(lax.ppermute(value.reshape(n_row, -1, LANES), "col", perm))
            return received

        dens = density.reshape(-1, extent)
        green = green_octant.reshape(-1, extent)
        begin = freqs // 2
        late_rows = (begin * n_row, freqs * n_row)
        late = z_forward_slots(col, dens, sin_z, late_rows, n_row, pairs)
        late = [late[0].reshape(n_row, -1, LANES), *send(late[1:])]
        first = z_forward([(green, *y_even, 0, freqs), (dens, *y_waves, 0, freqs)], n_dev, pairs)
        first = exchange(first)
        second = z_forward([(dens, *y_waves, extent, begin)], n_dev, pairs)
        second = exchange(second)
        late = join([late])
        late = spread(late).reshape(n_row, n_col, -1, pairs, LANES)
        kernel = kernel_planes(first, freqs, y_even, extent)

        def convolve(received, relative, offset, start, stop, joined):
            return convolve_planes(
                col, received, relative, offset, kernel, start, stop - start, joined, t_waves, y_waves, extent
            )

        own, *others = convolve(first, False, freqs, 0, freqs, False)
        cos_parts = [own.reshape(n_row, -1, LANES), *send(others)]
        parts = []
        for g, (start, stop) in enumerate(((0, begin), (begin, freqs))):
            (out,) = convolve(late if g else second, bool(g), 0, start, stop, True)
            out = spread(out)
            sent = send([out[:, s] for s in range(1, n_col)])
            parts.append(([out, *sent], sin_z, (start * n_row, stop * n_row)))
        cos_b = join([cos_parts])
        cos_b = lax.all_to_all(cos_b, "row", 0, 0)
        result = z_inverse(col, parts[:1], n_row, pairs, extent, None)
        cos_part = ([cos_b], cos_z, (0, freqs * n_row))
        result = z_inverse(col, [cos_part, parts[1]], n_row, pairs, extent, result)
        return result.reshape(local_x, local_y, extent)

    spec = P("row", "col", None)
    return jax.shard_map(on_device, mesh=mesh, in_specs=(spec, spec), out_specs=spec, check_vma=False)
```

```python
import numpy as np
import jax
import jax.numpy as jnp
from jax import lax
from jax.experimental import pallas as pl
from jax.experimental.pallas import tpu as pltpu
from jax.sharding import PartitionSpec as P


ALL = ("row", "col")
LANES = 128
BF16 = jnp.bfloat16
F32 = jnp.float32
NN = (((1,), (0,)), ((), ()))
NT = (((1,), (1,)), ((), ()))
TN = (((0,), (0,)), ((), ()))


def split_table(table):
    high = table.astype(np.float32).astype(jnp.bfloat16)
    low = (table - high.astype(np.float64)).astype(np.float32).astype(jnp.bfloat16)
    return high, low


def wave_tables(extent):
    freqs = np.arange(extent)[:, None] + 0.5
    cells = np.arange(extent)[None, :]
    angles = np.pi / extent * freqs * (cells - (extent - 1) / 2)
    waves = np.concatenate([np.cos(angles), np.sin(angles)], axis=0)
    weights = np.where(cells == 0, 1.0, 2.0)
    even = weights * np.cos(np.pi / extent * freqs * cells)
    return waves, even


def split(value):
    high = value.astype(BF16)
    low = (value - high.astype(F32)).astype(BF16)
    return high, low


def stack_left(high, low, axis):
    return jnp.concatenate([high, high, low], axis=axis)


def stack_right(high, low, axis):
    return jnp.concatenate([high, low, high], axis=axis)


def dot(left, right, dims):
    return lax.dot_general(left, right, dims, preferred_element_type=F32)


def whole(shape):
    return pl.BlockSpec(shape, lambda *_: (0,) * len(shape))


SCALAR = pl.BlockSpec(memory_space=pltpu.SMEM)
VECTOR = pl.BlockSpec(memory_space=pltpu.VMEM)


def z_forward(sources, n_dev, pairs):
    rows, extent = sources[0][0].shape
    all_planes = extent // n_dev
    counts = [source[4] for source in sources]
    width = sum(counts)
    per = min(8, pairs)
    n = len(sources)

    def body(*refs):
        out_ref = refs[-1]
        step = pl.program_id(0)
        for g in range(n):
            x_ref, h_ref, l_ref = refs[3 * g : 3 * g + 3]
            right = stack_right(*split(x_ref[...]), 1)
            part = slice(sources[g][3], sources[g][3] + extent)
            acc = dot(stack_left(h_ref[part, :], l_ref[part, :], 1), right, NT)
            for h in range(per):
                for d in range(n_dev):
                    start = (d * width + sum(counts[:g])) * pairs + per * step + h
                    out_ref[pl.ds(start, counts[g], stride=pairs), :] = acc[
                        d * all_planes : d * all_planes + counts[g], h * LANES : (h + 1) * LANES
                    ]

    lines = pl.BlockSpec((per * LANES, extent), lambda i: (i, 0))
    return pl.pallas_call(
        body,
        grid=(pairs // per,),
        in_specs=[s for source in sources for s in (lines, whole(source[1].shape), whole(source[2].shape))],
        out_specs=whole((n_dev * width * pairs, LANES)),
        out_shape=jax.ShapeDtypeStruct((n_dev * width * pairs, LANES), F32),
        cost_estimate=pl.CostEstimate(flops=6 * rows * extent * extent * n, transcendentals=0, bytes_accessed=8 * rows * extent * n),
        name="z_forward",
    )(*[a for source in sources for a in source[:3]])


def z_forward_slots(col, lines, tables, table_rows, n_row, pairs):
    rows, extent = lines.shape
    per = min(8, pairs)
    first, last = table_rows
    n_col = tables[0].shape[0]
    planes = (last - first) // n_row

    def body(col_ref, x_ref, h_ref, l_ref, *out_refs):
        step = pl.program_id(0)
        target = [lax.rem(col_ref[0] + s, n_col) for s in range(n_col)]
        high = jnp.concatenate([h_ref[c, first:last] for c in target], axis=0)
        low = jnp.concatenate([l_ref[c, first:last] for c in target], axis=0)
        acc = dot(stack_left(high, low, 1), stack_right(*split(x_ref[...]), 1), NT)
        for s, out_ref in enumerate(out_refs):
            for j in range(planes):
                row = (s * planes + j) * n_row
                for h in range(per):
                    start = j * pairs + per * step + h
                    out_ref[pl.ds(start, n_row, stride=planes * pairs), :] = acc[
                        row : row + n_row, h * LANES : (h + 1) * LANES
                    ]

    shape = (n_row * planes * pairs, LANES)
    return pl.pallas_call(
        body,
        grid=(pairs // per,),
        in_specs=[SCALAR, pl.BlockSpec((per * LANES, extent), lambda i: (i, 0))] + [whole(t.shape) for t in tables],
        out_specs=[whole(shape)] * n_col,
        out_shape=[jax.ShapeDtypeStruct(shape, F32)] * n_col,
        cost_estimate=pl.CostEstimate(
            flops=6 * rows * extent * n_col * (last - first), transcendentals=0, bytes_accessed=8 * rows * extent
        ),
        name="z_forward_slots",
    )(col, lines, *tables)


def z_inverse(col, groups, n_row, pairs, extent, partial):
    rows = pairs * LANES
    per = min(8, pairs)
    n_col = groups[0][1][0].shape[0]
    counts = [len(received) for received, _, _ in groups]
    depth = n_col * sum(last - first for _, _, (first, last) in groups)

    def body(col_ref, *refs):
        refs = list(refs)
        step = pl.program_id(0)
        source = [lax.rem(col_ref[0] + n_col - s, n_col) for s in range(n_col)]
        columns = [[] for _ in range(per)]
        highs, lows = [], []
        for g, (_, _, (first, last)) in enumerate(groups):
            r_refs = [refs.pop(0) for _ in range(counts[g])]
            h_ref, l_ref = refs.pop(0), refs.pop(0)
            planes = (last - first) // n_row
            for s in range(n_col):
                ref, slots, place = (r_refs[s], 1, 0) if s > 0 and len(r_refs) > 1 else (r_refs[0], n_col, s)
                for j in range(planes):
                    for h in range(per):
                        start = (place * planes + j) * pairs + per * step + h
                        columns[h].append(ref[pl.ds(start, n_row, stride=slots * planes * pairs), :])
                highs.append(h_ref[source[s], first:last])
                lows.append(l_ref[source[s], first:last])
        left = jnp.concatenate([jnp.concatenate(blocks, axis=0) for blocks in columns], axis=1)
        high = jnp.concatenate(highs, axis=0)
        low = jnp.concatenate(lows, axis=0)
        acc = dot(stack_right(*split(left), 0), stack_left(high, low, 0), TN)
        if partial is not None:
            acc = acc + refs[0][...]
        refs[-1][...] = acc

    lines = pl.BlockSpec((per * LANES, extent), lambda i: (i, 0))
    specs, operands = [SCALAR], [col]
    for received, tables, _ in groups:
        specs += [VECTOR] * len(received) + [whole(t.shape) for t in tables]
        operands += [r.reshape(-1, LANES) for r in received] + list(tables)
    if partial is not None:
        specs.append(lines)
        operands.append(partial)
    return pl.pallas_call(
        body,
        grid=(pairs // per,),
        in_specs=specs,
        out_specs=lines,
        out_shape=jax.ShapeDtypeStruct((rows, extent), F32),
        cost_estimate=pl.CostEstimate(
            flops=6 * rows * extent * depth, transcendentals=0, bytes_accessed=8 * rows * extent
        ),
        name="z_inverse",
    )(*operands)


def lane_half(shape):
    return lax.broadcasted_iota(jnp.int32, shape, 1) < LANES // 2


def swap(value):
    return pltpu.roll(value, LANES // 2, 1)


def read_plane(ref, index, plane_ref, slot=lambda c: c):
    n_row, n_col, _, pairs, _ = ref.shape
    half_x = n_row * pairs
    mask = lane_half((half_x, LANES))
    for p in range(n_col // 2):
        a = ref[:, slot(2 * p), index].reshape(half_x, LANES)
        b = ref[:, slot(2 * p + 1), index].reshape(half_x, LANES)
        plane_ref[p, pl.ds(0, half_x, stride=2)] = jnp.where(mask, a, swap(b))
        plane_ref[p, pl.ds(1, half_x, stride=2)] = jnp.where(mask, swap(a), b)
    return jnp.concatenate([plane_ref[p] for p in range(n_col // 2)], axis=1)


def write_plane(col, plane, plane_ref, block_ref, store):
    n_col = block_ref.shape[0]
    half_x = plane_ref.shape[1] // 2
    mask = lane_half((half_x, LANES))
    for p in range(n_col // 2):
        plane_ref[p] = plane[:, p * LANES : (p + 1) * LANES]
        q0 = plane_ref[p, pl.ds(0, half_x, stride=2)]
        q1 = plane_ref[p, pl.ds(1, half_x, stride=2)]
        block_ref[2 * p] = jnp.where(mask, q0, swap(q1))
        block_ref[2 * p + 1] = jnp.where(mask, swap(q0), q1)
    for s in range(n_col):
        store(s, block_ref[lax.rem(col + s, n_col)])


def kernel_planes(received, planes, tables, extent):
    scaling = 1.0 / float(extent) ** 3
    per = min(4, planes)

    def body(r_ref, yh, yl, out_ref, plane_ref):
        for i in range(per):
            plane = read_plane(r_ref, per * pl.program_id(0) + i, plane_ref.at[i])
            first = dot(stack_left(yh[...], yl[...], 1), stack_right(*split(plane), 0), NN)
            second = dot(stack_left(*split(first), 1), stack_right(yh[...], yl[...], 1), NT)
            out_ref[i] = second * scaling

    return pl.pallas_call(
        body,
        grid=(planes // per,),
        in_specs=[VECTOR] + [whole(t.shape) for t in tables],
        out_specs=pl.BlockSpec((per, extent, extent), lambda k: (k, 0, 0)),
        out_shape=jax.ShapeDtypeStruct((planes, extent, extent), F32),
        scratch_shapes=[pltpu.VMEM((per, extent // LANES, extent, LANES), F32)],
        cost_estimate=pl.CostEstimate(flops=12 * planes * extent**3, transcendentals=0, bytes_accessed=8 * planes * extent**2),
        name="kernel_planes",
    )(received, *tables)


def convolve_planes(col, received, relative, offset, kernel, kernel_offset, planes, joined, t_tables, y_tables, extent):
    n_row, n_col, _, pairs, _ = received.shape

    per = 2 if planes % 2 == 0 else 1

    def body(col_ref, r_ref, k_ref, th, tl, yh, yl, *rest):
        *outs, plane_ref, block_ref = rest
        slot = (lambda c: lax.rem(col_ref[0] + (n_col - c), n_col)) if relative else (lambda c: c)
        results = []
        for i in range(per):
            plane = read_plane(r_ref, offset + per * pl.program_id(0) + i, plane_ref.at[i], slot)
            along_x = dot(stack_left(yh[...], yl[...], 1), stack_right(*split(plane), 0), NN)
            along_y = []
            for row in range(0, 2 * extent, LANES):
                part = along_x[row : row + LANES]
                weight = k_ref[i, row % extent : row % extent + LANES, :]
                weight = jnp.concatenate([weight, weight], axis=1)
                spectrum = dot(stack_left(*split(part), 1), stack_right(th[...], tl[...], 0), NN) * weight
                along_y.append(dot(stack_left(*split(spectrum), 1), stack_right(yh[...], yl[...], 0), NN))
            along_y = jnp.concatenate(along_y, axis=0)
            results.append(dot(stack_left(th[...], tl[...], 1), stack_right(*split(along_y), 0), NN))

        for i in range(per):

            def store(s, value):
                value = value.reshape(n_row, pairs, LANES)
                if joined:
                    outs[0][:, s, i] = value
                else:
                    outs[s][:, i] = value

            write_plane(col_ref[0], results[i], plane_ref.at[i], block_ref, store)

    tables = (*t_tables, *y_tables)
    if joined:
        shapes = [(n_row, n_col, planes, pairs, LANES)]
        specs = [pl.BlockSpec((n_row, n_col, per, pairs, LANES), lambda k: (0, 0, k, 0, 0))]
    else:
        shapes = [(n_row, planes, pairs, LANES)] * n_col
        specs = [pl.BlockSpec((n_row, per, pairs, LANES), lambda k: (0, k, 0, 0))] * n_col
    return pl.pallas_call(
        body,
        grid=(planes // per,),
        in_specs=[SCALAR, VECTOR, pl.BlockSpec((per, extent, extent), lambda k: (kernel_offset // per + k, 0, 0))]
        + [whole(t.shape) for t in tables],
        out_specs=specs,
        out_shape=[jax.ShapeDtypeStruct(s, F32) for s in shapes],
        scratch_shapes=[
            pltpu.VMEM((per, extent // LANES, extent, LANES), F32),
            pltpu.VMEM((n_col, n_row * pairs, LANES), F32),
        ],
        cost_estimate=pl.CostEstimate(flops=72 * planes * extent**3, transcendentals=0, bytes_accessed=12 * planes * extent**2),
        name="convolve_planes",
    )(col, received, kernel, *tables)


def join(groups):
    n_row = groups[0][0].shape[0]
    lengths = [group[0].shape[1] for group in groups]
    n_slot = len(groups[0])
    block = n_row // 2

    def body(*refs):
        begin = 0
        for g, length in enumerate(lengths):
            for s in range(n_slot):
                refs[-1][:, s, begin : begin + length] = refs[g * n_slot + s][...]
            begin += length

    total = sum(lengths)
    return pl.pallas_call(
        body,
        grid=(n_row // block,),
        in_specs=[pl.BlockSpec((block, n, LANES), lambda i: (i, 0, 0)) for n in lengths for _ in range(n_slot)],
        out_specs=pl.BlockSpec((block, n_slot, total, LANES), lambda i: (i, 0, 0, 0)),
        out_shape=jax.ShapeDtypeStruct((n_row, n_slot, total, LANES), F32),
        name="join",
    )(*[part for group in groups for part in group])


def solution(mesh):
    n_row, n_col = mesh.shape["row"], mesh.shape["col"]
    n_dev = n_row * n_col

    def on_device(density, green_octant):
        local_x, local_y, extent = density.shape
        pairs = local_x * local_y // LANES
        freqs = extent // n_dev
        waves, even = wave_tables(extent)
        y_waves = split_table(waves)
        t_waves = split_table(waves.T)
        y_even = split_table(even)

        def by_owner(table):
            table = table.reshape(n_row, n_col, freqs, extent).transpose(1, 2, 0, 3)
            return table.reshape(n_col, freqs * n_row, extent)

        cos_z = split_table(by_owner(waves[:extent]))
        sin_z = split_table(by_owner(waves[extent:]))
        col = lax.axis_index("col").astype(jnp.int32).reshape(1)

        def exchange(value):
            value = lax.all_to_all(value.reshape(n_dev, -1, LANES), ALL, 0, 0)
            return value.reshape(n_row, n_col, -1, pairs, LANES)

        def spread(value):
            return lax.all_to_all(value.reshape(n_row, n_col, -1, LANES), "row", 0, 0)

        def send(values):
            received = []
            for s, value in enumerate(values, start=1):
                perm = [(c, (c + s) % n_col) for c in range(n_col)]
                received.append(lax.ppermute(value.reshape(n_row, -1, LANES), "col", perm))
            return received

        dens = density.reshape(-1, extent)
        green = green_octant.reshape(-1, extent)
        begin = freqs // 2
        late_rows = (begin * n_row, freqs * n_row)
        late = z_forward_slots(col, dens, sin_z, late_rows, n_row, pairs)
        late = [late[0].reshape(n_row, -1, LANES), *send(late[1:])]
        first = z_forward([(green, *y_even, 0, freqs), (dens, *y_waves, 0, freqs)], n_dev, pairs)
        first = exchange(first)
        second = z_forward([(dens, *y_waves, extent, begin)], n_dev, pairs)
        second = exchange(second)
        late = join([late])
        late = spread(late).reshape(n_row, n_col, -1, pairs, LANES)
        kernel = kernel_planes(first, freqs, y_even, extent)

        def convolve(received, relative, offset, start, stop, joined):
            return convolve_planes(
                col, received, relative, offset, kernel, start, stop - start, joined, t_waves, y_waves, extent
            )

        own, *others = convolve(first, False, freqs, 0, freqs, False)
        cos_parts = [own.reshape(n_row, -1, LANES), *send(others)]
        parts = []
        for g, (start, stop) in enumerate(((0, begin), (begin, freqs))):
            (out,) = convolve(late if g else second, bool(g), 0, start, stop, True)
            out = spread(out)
            sent = send([out[:, s] for s in range(1, n_col)])
            parts.append(([out, *sent], sin_z, (start * n_row, stop * n_row)))
        cos_b = join([cos_parts])
        cos_b = lax.all_to_all(cos_b, "row", 0, 0)
        result = z_inverse(col, parts[:1], n_row, pairs, extent, None)
        cos_part = ([cos_b], cos_z, (0, freqs * n_row))
        result = z_inverse(col, [cos_part, parts[1]], n_row, pairs, extent, result)
        return result.reshape(local_x, local_y, extent)

    spec = P("row", "col", None)
    return jax.shard_map(on_device, mesh=mesh, in_specs=(spec, spec), out_specs=spec, check_vma=False)
```
